32 devices in a mesh: grp: 4 (over z), freq: 8 (over y, x, core).
Axes of the slice: x: 2, y: 2, z: 4, core: 2. Of those that a mesh axis runs over, the one named last changes fastest.
Arguments:
- sources: bfloat16 [1024, 32768], P('freq', 'grp'), may hold values from -6 to 6
- panel_pos: float32 [3, 32768], P(None, 'grp'), may hold values from -1 to 1
- panel_blade: int32 [32768], P('grp'), may hold values from 0 to 3
- observer_table: float32 [3, 2048], replicated, may hold values from -8 to 8, as said below
- observer_index: int32 [32], replicated, may hold values from 0 to 2047
Outputs:
- spectra: float32 [512, 4, 2, 32], P('freq', 'grp')
The draws below stay inside these ranges and needn't reach their ends.
Inputs may be any that keep to these rules, and one draw needn't show every extreme that they name: `observer_table`: each observer lies 3 to 8 units from the anchor (0, 0, 0).
All inputs are finite; a program needn't handle non-finite values.
Results may differ from the reference program's by a relative error of at most 0.0047.
Values may be sent and summed in bfloat16 or wider, within the bound.
A program may use at most 64 MiB of HBM per device.

```python
import math
import jax
import jax.numpy as jnp
from jax import lax

NT = 1024
NF = 512
NCOMP = 4
NOBS = 32
NOBS_ALL = 2048
PANELS = 32768


def draw_observer_table(key, part):
    key_height = jax.random.fold_in(key, 11)
    key_turn = jax.random.fold_in(key, 12)
    key_radius = jax.random.fold_in(key, 13)
    height = jax.random.uniform(key_height, (NOBS_ALL,), jnp.float32, -1.0, 1.0)
    turn_angle = jax.random.uniform(key_turn, (NOBS_ALL,), jnp.float32, -math.pi, math.pi)
    uniform_part = jax.random.uniform(key_radius, (NOBS_ALL,), jnp.float32, 0.0, 1.0)
    radius = 3.0 + 5.0 * uniform_part
    cycle_radius = jnp.sqrt(jnp.maximum(1.0 - height * height, 0.0))
    return jnp.stack([radius * cycle_radius * jnp.cos(turn_angle), radius * cycle_radius * jnp.sin(turn_angle), radius * height]).astype(jnp.float32)


def place_ends(result, own_key, least, largest):
    spot = [jax.random.randint(jax.random.fold_in(own_key, axis), (), 0, length) for axis, length in enumerate(result.shape)]
    widest = result.shape.index(max(result.shape))
    beside = spot[:widest] + [(spot[widest] + 1) % result.shape[widest]] + spot[widest + 1:]
    return result.at[tuple(spot)].set(least).at[tuple(beside)].set(largest)


def level_of(rng, dims, shards, low, largest):
    gain = 1.0
    for position, blocks in shards:
        draws = jax.random.uniform(jax.random.fold_in(jax.random.fold_in(rng, 6), position), (blocks,), jnp.float32, low / len(shards), largest / len(shards))
        gain = gain * jnp.repeat(jnp.exp(draws), dims[position] // blocks).reshape((-1,) + (1,) * (len(dims) - 1 - position))
    return gain


def normal_values(own_key, shape, deviation, limit, split=(), kind=jnp.bfloat16):
    drawn = deviation * jax.random.normal(own_key, shape, jnp.float32)
    if split:
        drawn = drawn * level_of(own_key, shape, split, -0.22, 0.18)
    return jnp.clip(drawn, -limit, limit).astype(kind)


def setup_inputs(seed: int = 0) -> dict:
    arg_keys = jax.random.split(jax.random.key(seed), 6)
    return {
        "sources": normal_values(arg_keys[0], (NT, PANELS), 1.0, 6.0, ((0, 8), (1, 4))),
        "panel_pos": jnp.clip(jax.random.uniform(arg_keys[1], (3, PANELS), jnp.float32, -1.0, 1.0) * level_of(arg_keys[1], (3, PANELS), ((1, 4),), -0.4, 0.0), -1.0, 1.0),
        "panel_blade": place_ends(jax.random.randint(arg_keys[2], (PANELS,), 0, NCOMP), jax.random.fold_in(arg_keys[2], 1), 0, NCOMP - 1).astype(jnp.int32),
        "observer_table": draw_observer_table(jax.random.fold_in(arg_keys[5], 71), 0),
        "observer_index": place_ends(jax.random.randint(arg_keys[4], (NOBS,), 0, NOBS_ALL), jax.random.fold_in(arg_keys[4], 1), 0, NOBS_ALL - 1).astype(jnp.int32),
    }


wave_step = 0.04

def transform_table():
    row_index = jnp.arange(2 * NF, dtype=jnp.int32)
    samples = jnp.arange(NT, dtype=jnp.int32)
    frequency = row_index // 2
    parity = row_index % 2
    turn_count = frequency[:, None] * samples[None, :] % NT
    angle_table = 2.0 * math.pi / NT * turn_count.astype(jnp.float32)
    values = jnp.where(parity[:, None] == 0, jnp.cos(angle_table), -jnp.sin(angle_table))
    return (values / math.sqrt(NT)).astype(jnp.bfloat16)

def distances(positions, observers):
    offset_x = observers[0][:, None] - positions[0][None, :]
    offset_y = observers[1][:, None] - positions[1][None, :]
    offset_z = observers[2][:, None] - positions[2][None, :]
    return jnp.sqrt(offset_x * offset_x + offset_y * offset_y + offset_z * offset_z)

def blade_masks(blades):
    return (blades[None, :] == jnp.arange(NCOMP, dtype=jnp.int32)[:, None]).astype(jnp.bfloat16)

def frequency_term(frequency, spectrum_pair, blade_mask, distance, amplitude):
    wavenumber = wave_step * frequency.astype(jnp.float32)
    phase_angle = wavenumber * distance
    green_matrix = jnp.concatenate([jnp.cos(phase_angle) * amplitude, -jnp.sin(phase_angle) * amplitude], axis=0).astype(jnp.bfloat16)
    weighted = jnp.concatenate([spectrum_pair[0][None, :] * blade_mask, spectrum_pair[1][None, :] * blade_mask], axis=0)
    product = lax.dot_general(weighted, green_matrix, (((1,), (1,)), ((), ())), preferred_element_type=jnp.float32)
    blade_count = blade_mask.shape[0]
    observer_count = distance.shape[0]
    real_part = product[:blade_count, :observer_count] - product[blade_count:, observer_count:]
    imag_part = product[:blade_count, observer_count:] + product[blade_count:, :observer_count]
    return jnp.stack([real_part, imag_part], axis=1)

def reference(sources, panel_pos, panel_blade, observer_table, observer_index):
    observers = observer_table[:, observer_index]
    spectrum = jnp.dot(transform_table(), sources, preferred_element_type=jnp.float32).astype(jnp.bfloat16)
    spectrum = spectrum.reshape(NF, 2, spectrum.shape[1])
    distance = distances(panel_pos, observers)
    amplitude = 0.25 / (math.pi * distance)
    blade_mask = blade_masks(panel_blade)

    def per_frequency(element):
        return frequency_term(element[0], element[1], blade_mask, distance, amplitude)
    return lax.map(per_frequency, (jnp.arange(NF, dtype=jnp.int32), spectrum))
```

```python
import functools
import math

import jax
import jax.numpy as jnp
import numpy as np
from jax import lax
from jax.experimental import pallas as pl
from jax.experimental.pallas import tpu as pltpu
from jax.sharding import PartitionSpec as P

NT = 1024
NF = 512
NCOMP = 4
WAVE_STEP = 0.04
LANES = 128
CHUNK = 256
STEPS = 8


def transform_table():
    turns = (np.arange(NF)[:, None] * np.arange(NT)[None, :]) % NT
    angle = 2.0 * math.pi / NT * turns
    values = np.stack([np.cos(angle), -np.sin(angle)], axis=1).reshape(2 * NF, NT)
    return jnp.asarray((values / math.sqrt(NT)).astype(np.float32)).astype(jnp.bfloat16)


def cos_sin(x):
    y = x * x
    cos = jnp.full_like(y, 1.0 / math.factorial(16))
    sin = jnp.full_like(y, -1.0 / math.factorial(15))
    for n in range(7, -1, -1):
        sign = 1.0 if n % 2 == 0 else -1.0
        cos = cos * y + sign / math.factorial(2 * n)
        if n < 7:
            sin = sin * y + sign / math.factorial(2 * n + 1)
    return cos, sin * x


def start_states(pos_ref, obs_ref, states, row0, share):
    rows = 32
    lane = lax.broadcasted_iota(jnp.int32, (rows, LANES), 1)
    j = (lane // (LANES // share)).astype(jnp.float32)
    for r in range(CHUNK // rows):
        at = pl.ds(row0 + r * rows, rows)
        d2 = None
        for axis in range(3):
            diff = obs_ref[axis : axis + 1, :] - pos_ref[at, axis : axis + 1]
            d2 = diff * diff if d2 is None else d2 + diff * diff
        d = jnp.sqrt(d2)
        amplitude = 0.25 / (math.pi * d)
        theta = WAVE_STEP * d
        cj, sj = cos_sin(j * theta)
        cs, ss = cos_sin(float(share) * theta)
        cj, sj = cj * amplitude, sj * amplitude
        out = pl.ds(r * rows, rows)
        states[0, out, :] = cj * cs + sj * ss
        states[1, out, :] = cj
        states[2, out, :] = sj * cs - cj * ss
        states[3, out, :] = sj
        states[4, out, :] = 2.0 * cs


def green_rows(states, green, r):
    at = pl.ds(r * 16, 16)
    c0, c1, s0, s1, t = (states[i, at, :] for i in range(5))
    for k in range(STEPS):
        green[k, at, :LANES] = c1.astype(jnp.bfloat16)
        green[k, at, LANES:] = s1.astype(jnp.bfloat16)
        c0, c1 = c1, t * c1 - c0
        s0, s1 = s1, t * s1 - s0
    states[0, at, :], states[1, at, :] = c0, c1
    states[2, at, :], states[3, at, :] = s0, s1


def contract(spec, mask, green, acc, step, k, share, first):
    sub = lax.broadcasted_iota(jnp.int32, (2 * NCOMP, CHUNK), 0)
    real_row = sub < NCOMP
    rows = []
    base = pl.multiple_of(step * 2 * share, 2 * share)
    pair = spec[pl.ds(base, 2 * share), :]
    for j in range(share):
        re = jnp.broadcast_to(pair[2 * j : 2 * j + 1, :], (2 * NCOMP, CHUNK))
        im = jnp.broadcast_to(pair[2 * j + 1 : 2 * j + 2, :], (2 * NCOMP, CHUNK))
        rows.append(jnp.where(real_row, re, im) * mask)
    weighted = jnp.concatenate(rows, axis=0).astype(jnp.bfloat16)
    prod = jnp.dot(weighted, green[k], preferred_element_type=jnp.float32)
    lane = lax.broadcasted_iota(jnp.int32, (2 * NCOMP, LANES), 1) // (LANES // share)
    even = prod[: 2 * NCOMP, :LANES]
    odd = prod[: 2 * NCOMP, LANES:]
    for j in range(1, share):
        block = prod[2 * NCOMP * j : 2 * NCOMP * (j + 1)]
        even = jnp.where(lane == j, block[:, :LANES], even)
        odd = jnp.where(lane == j, block[:, LANES:], odd)
    odd = jnp.concatenate([odd[NCOMP:], -odd[:NCOMP]], axis=0)
    total = even + odd
    if first:
        acc[step] = total
    else:
        acc[step] = acc[step] + total


def block_pair(spec, mask, now, acc, block, share, first, states, later):
    per = CHUNK // 16 // STEPS
    for k in range(STEPS):
        if now is not None:
            contract(spec, mask, now, acc, block * STEPS + k, k, share, first)
        if later is not None:
            for r in range(per):
                green_rows(states, later, k * per + r)


def phase(q, first, table_ref, block_of, pos_ref, blade_ref, obs_ref, acc, spec, states, mask, ga, gb, share):
    row0 = pl.multiple_of(q * CHUNK, CHUNK)
    start_states(pos_ref, obs_ref, states, row0, share)
    sub = lax.broadcasted_iota(jnp.int32, (2 * NCOMP, CHUNK), 0) % NCOMP
    mask[...] = jnp.where(blade_ref[:, pl.ds(row0, CHUNK)] == sub, 1.0, 0.0)
    block_pair(None, None, None, None, 0, share, first, states, ga)
    data = block_of(q)
    for r in range(4):
        part = pl.ds(r * (2 * NF // 4), 2 * NF // 4)
        spec[part, :] = (
            jnp.dot(table_ref[part, :], data, preferred_element_type=jnp.float32)
            .astype(jnp.bfloat16)
            .astype(jnp.float32)
        )
    blocks = NF // share // STEPS
    m = mask[...]

    def two(i, carry):
        block_pair(spec, m, ga, acc, 2 * i, share, first, states, gb)
        block_pair(spec, m, gb, acc, 2 * i + 1, share, first, states, ga)
        return carry

    lax.fori_loop(0, blocks // 2, two, 0)


def kernel(share, table_ref, data_ref, pos_ref, blade_ref, obs_ref, acc, spec, states, mask, ga, gb):
    def block_of(q):
        return data_ref[:, pl.ds(pl.multiple_of(q * CHUNK, CHUNK), CHUNK)]

    acc[...] = jnp.zeros_like(acc)

    def step(q, carry):
        phase(q, False, table_ref, block_of, pos_ref, blade_ref, obs_ref, acc, spec, states, mask, ga, gb, share)
        return carry

    lax.fori_loop(0, data_ref.shape[1] // CHUNK, step, 0)


def body(sources, panel_pos, panel_blade, observer_table, observer_index):
    nfreq, ngrp = lax.axis_size("freq"), lax.axis_size("grp")
    me = lax.axis_index("freq")
    nobs = observer_index.shape[0]
    share = LANES // nobs
    panels = sources.shape[1] // nfreq
    observers = jnp.tile(observer_table[:, observer_index], (1, share))
    pos = lax.dynamic_slice_in_dim(panel_pos, me * panels, panels, 1).T
    blade = lax.dynamic_slice_in_dim(panel_blade, me * panels, panels, 0)[None, :]
    shaped = sources.reshape(sources.shape[0], nfreq, panels)
    piece = lax.all_to_all(shaped, "freq", split_axis=1, concat_axis=0, tiled=True).reshape(NT, panels)
    steps = NF // share
    partial = pl.pallas_call(
        functools.partial(kernel, share),
        out_shape=jax.ShapeDtypeStruct((steps, 2 * NCOMP, LANES), jnp.float32),
        in_specs=[pl.BlockSpec(memory_space=pltpu.VMEM)] * 5,
        out_specs=pl.BlockSpec(memory_space=pltpu.VMEM),
        scratch_shapes=[
            pltpu.VMEM((2 * NF, CHUNK), jnp.float32),
            pltpu.VMEM((5, CHUNK, LANES), jnp.float32),
            pltpu.VMEM((2 * NCOMP, CHUNK), jnp.float32),
            pltpu.VMEM((STEPS, CHUNK, 2 * LANES), jnp.bfloat16),
            pltpu.VMEM((STEPS, CHUNK, 2 * LANES), jnp.bfloat16),
        ],
    )(transform_table(), piece, pos, blade, observers)
    mine = steps // nfreq
    parts = lax.all_to_all(partial.reshape(nfreq, mine, 2 * NCOMP, LANES), "freq", split_axis=0, concat_axis=0, tiled=True)
    summed = jnp.sum(parts, axis=0)
    blades = summed.reshape(mine, 2, ngrp, NCOMP // ngrp, LANES).transpose(2, 0, 1, 3, 4)
    got = jnp.sum(lax.all_to_all(blades, "grp", split_axis=0, concat_axis=0, tiled=True), axis=0)
    got = got.reshape(mine, 2, NCOMP // ngrp, share, nobs).transpose(0, 3, 2, 1, 4)
    return got.reshape(mine * share, NCOMP // ngrp, 2, nobs)


def solution(mesh):
    in_specs = (P("freq", "grp"), P(None, "grp"), P("grp"), P(), P())
    out_specs = P("freq", "grp", None, None)
    return jax.shard_map(body, mesh=mesh, in_specs=in_specs, out_specs=out_specs, check_vma=False)
```

```python
import functools
import math

import jax
import jax.numpy as jnp
import numpy as np
from jax import lax
from jax.experimental import pallas as pl
from jax.experimental.pallas import tpu as pltpu
from jax.sharding import PartitionSpec as P

NT = 1024
NF = 512
NCOMP = 4
WAVE_STEP = 0.04
MESH = pl.DeviceIdType.MESH
LANES = 128
CHUNK = 256
STEPS = 8


def transform_table():
    turns = (np.arange(NF)[:, None] * np.arange(NT)[None, :]) % NT
    angle = 2.0 * math.pi / NT * turns
    values = np.stack([np.cos(angle), -np.sin(angle)], axis=1).reshape(2 * NF, NT)
    return jnp.asarray((values / math.sqrt(NT)).astype(np.float32)).astype(jnp.bfloat16)


def cos_sin(x):
    y = x * x
    cos = jnp.full_like(y, 1.0 / math.factorial(16))
    sin = jnp.full_like(y, -1.0 / math.factorial(15))
    for n in range(7, -1, -1):
        sign = 1.0 if n % 2 == 0 else -1.0
        cos = cos * y + sign / math.factorial(2 * n)
        if n < 7:
            sin = sin * y + sign / math.factorial(2 * n + 1)
    return cos, sin * x


def start_states(pos_ref, obs_ref, states, row0, share):
    rows = 32
    lane = lax.broadcasted_iota(jnp.int32, (rows, LANES), 1)
    j = (lane // (LANES // share)).astype(jnp.float32)
    for r in range(CHUNK // rows):
        at = pl.ds(row0 + r * rows, rows)
        d2 = None
        for axis in range(3):
            diff = obs_ref[axis : axis + 1, :] - pos_ref[at, axis : axis + 1]
            d2 = diff * diff if d2 is None else d2 + diff * diff
        d = jnp.sqrt(d2)
        amplitude = 0.25 / (math.pi * d)
        theta = WAVE_STEP * d
        cj, sj = cos_sin(j * theta)
        cs, ss = cos_sin(float(share) * theta)
        cj, sj = cj * amplitude, sj * amplitude
        out = pl.ds(r * rows, rows)
        states[0, out, :] = cj * cs + sj * ss
        states[1, out, :] = cj
        states[2, out, :] = sj * cs - cj * ss
        states[3, out, :] = sj
        states[4, out, :] = 2.0 * cs


def green_rows(states, green, r):
    at = pl.ds(r * 16, 16)
    c0, c1, s0, s1, t = (states[i, at, :] for i in range(5))
    for k in range(STEPS):
        green[k, at, :LANES] = c1.astype(jnp.bfloat16)
        green[k, at, LANES:] = s1.astype(jnp.bfloat16)
        c0, c1 = c1, t * c1 - c0
        s0, s1 = s1, t * s1 - s0
    states[0, at, :], states[1, at, :] = c0, c1
    states[2, at, :], states[3, at, :] = s0, s1


def contract(spec, mask, green, acc, step, k, share, first):
    sub = lax.broadcasted_iota(jnp.int32, (2 * NCOMP, CHUNK), 0)
    real_row = sub < NCOMP
    rows = []
    base = pl.multiple_of(step * 2 * share, 2 * share)
    pair = spec[pl.ds(base, 2 * share), :]
    for j in range(share):
        re = jnp.broadcast_to(pair[2 * j : 2 * j + 1, :], (2 * NCOMP, CHUNK))
        im = jnp.broadcast_to(pair[2 * j + 1 : 2 * j + 2, :], (2 * NCOMP, CHUNK))
        rows.append(jnp.where(real_row, re, im) * mask)
    weighted = jnp.concatenate(rows, axis=0).astype(jnp.bfloat16)
    prod = jnp.dot(weighted, green[k], preferred_element_type=jnp.float32)
    lane = lax.broadcasted_iota(jnp.int32, (2 * NCOMP, LANES), 1) // (LANES // share)
    even = prod[: 2 * NCOMP, :LANES]
    odd = prod[: 2 * NCOMP, LANES:]
    for j in range(1, share):
        block = prod[2 * NCOMP * j : 2 * NCOMP * (j + 1)]
        even = jnp.where(lane == j, block[:, :LANES], even)
        odd = jnp.where(lane == j, block[:, LANES:], odd)
    odd = jnp.concatenate([odd[NCOMP:], -odd[:NCOMP]], axis=0)
    total = even + odd
    if first:
        acc[step] = total
    else:
        acc[step] = acc[step] + total


def block_pair(spec, mask, now, acc, block, share, first, states, later):
    per = CHUNK // 16 // STEPS
    for k in range(STEPS):
        if now is not None:
            contract(spec, mask, now, acc, block * STEPS + k, k, share, first)
        if later is not None:
            for r in range(per):
                green_rows(states, later, k * per + r)


def phase(q, first, table_ref, block_of, pos_ref, blade_ref, obs_ref, acc, spec, states, mask, ga, gb, share, done):
    row0 = pl.multiple_of(q * CHUNK, CHUNK)
    start_states(pos_ref, obs_ref, states, row0, share)
    sub = lax.broadcasted_iota(jnp.int32, (2 * NCOMP, CHUNK), 0) % NCOMP
    mask[...] = jnp.where(blade_ref[:, pl.ds(row0, CHUNK)] == sub, 1.0, 0.0)
    block_pair(None, None, None, None, 0, share, first, states, ga)
    data = block_of(q)
    for r in range(4):
        part = pl.ds(r * (2 * NF // 4), 2 * NF // 4)
        spec[part, :] = (
            jnp.dot(table_ref[part, :], data, preferred_element_type=jnp.float32)
            .astype(jnp.bfloat16)
            .astype(jnp.float32)
        )
    blocks = NF // share // STEPS
    m = mask[...]

    def two(i, carry):
        block_pair(spec, m, ga, acc, 2 * i, share, first, states, gb)
        block_pair(spec, m, gb, acc, 2 * i + 1, share, first, states, ga)
        done(q, i)
        return carry

    lax.fori_loop(0, blocks // 2, two, 0)


def kernel(share, size, table_ref, src_ref, pos_ref, blade_ref, obs_ref, out_ref, *scratch):
    (acc, spec, states, mask, ga, gb, data, parts, total, zsend, zrecv) = scratch[:11]
    (send_sem, recv_sem, part_send, part_recv, z_send, z_recv) = scratch[11:]
    nfreq, ngrp = size
    me, grp = lax.axis_index("freq"), lax.axis_index("grp")
    rows = src_ref.shape[0]
    panels = src_ref.shape[1] // nfreq
    chunks = panels // CHUNK
    mine = NF // share // nfreq

    def freq_peer(d):
        return lax.rem(me + d, nfreq)

    barrier = pltpu.get_barrier_semaphore()

    def greet(d, carry):
        pl.semaphore_signal(barrier, inc=1, device_id={"freq": freq_peer(d)}, device_id_type=MESH)
        return carry

    lax.fori_loop(1, nfreq, greet, 0)
    for d in range(1, ngrp):
        pl.semaphore_signal(barrier, inc=1, device_id={"grp": lax.rem(grp + d, ngrp)}, device_id_type=MESH)
    pl.semaphore_wait(barrier, nfreq + ngrp - 2)

    def columns(owner, q):
        return pl.ds(pl.multiple_of(owner * panels + q * CHUNK, CHUNK), CHUNK)

    landing = pl.ds(pl.multiple_of(me * rows, rows), rows)

    def send_chunk(q, carry):
        def to(d, carry):
            dest = freq_peer(d)
            pltpu.make_async_remote_copy(
                src_ref=src_ref.at[:, columns(dest, q)],
                dst_ref=data.at[q, landing, :],
                send_sem=send_sem.at[q],
                recv_sem=recv_sem.at[q],
                device_id={"freq": dest},
                device_id_type=MESH,
            ).start()
            return carry

        lax.fori_loop(1, nfreq, to, 0)
        pltpu.make_async_copy(src_ref.at[:, columns(me, q)], data.at[q, landing, :], recv_sem.at[q]).start()
        return carry

    lax.fori_loop(0, chunks, send_chunk, 0)
    acc[...] = jnp.zeros_like(acc)

    def block_of(q):
        pltpu.make_async_copy(data.at[q], data.at[q], recv_sem.at[q]).wait()
        return data[q]

    def done(q, i):
        ranges = 2 * STEPS // mine

        @pl.when(q == chunks - 1)
        def _():
            for r in range(ranges):
                dest = i * ranges + r

                @pl.when(dest != me)
                def _():
                    pltpu.make_async_remote_copy(
                        src_ref=acc.at[pl.ds(dest * mine, mine)],
                        dst_ref=parts.at[me],
                        send_sem=part_send,
                        recv_sem=part_recv,
                        device_id={"freq": dest},
                        device_id_type=MESH,
                    ).start()

    def step(q, carry):
        phase(q, False, table_ref, block_of, pos_ref, blade_ref, obs_ref, acc, spec, states, mask, ga, gb, share, done)
        return carry

    lax.fori_loop(0, chunks, step, 0)

    parts[me] = acc[pl.ds(me * mine, mine)]
    others = parts.at[pl.ds(0, nfreq - 1)]
    pltpu.make_async_copy(others, others, part_recv).wait()
    total[...] = jnp.sum(parts[...], axis=0)
    held = NCOMP // ngrp
    for g in range(ngrp):
        for b in range(held):
            for c in range(2):
                at = (b * 2 + c) * mine
                zsend[g, at : at + mine, :] = total[:, c * NCOMP + g * held + b, :]
    for d in range(1, ngrp):
        dest = lax.rem(grp + d, ngrp)
        pltpu.make_async_remote_copy(
            src_ref=zsend.at[dest],
            dst_ref=zrecv.at[grp],
            send_sem=z_send,
            recv_sem=z_recv,
            device_id={"grp": dest},
            device_id_type=MESH,
        ).start()
    zrecv[grp] = zsend[grp]
    rest = zrecv.at[pl.ds(0, ngrp - 1)]
    pltpu.make_async_copy(rest, rest, z_recv).wait()
    out_ref[...] = jnp.sum(zrecv[...], axis=0)
    pltpu.make_async_copy(rest, rest, z_send).wait()
    pltpu.make_async_copy(others, others, part_send).wait()

    def drain(q, carry):
        sent = data.at[q, pl.ds(0, (nfreq - 1) * rows), :]
        pltpu.make_async_copy(sent, sent, send_sem.at[q]).wait()
        return carry

    lax.fori_loop(0, chunks, drain, 0)


def body(sources, panel_pos, panel_blade, observer_table, observer_index):
    nfreq, ngrp = lax.axis_size("freq"), lax.axis_size("grp")
    me = lax.axis_index("freq")
    nobs = observer_index.shape[0]
    share = LANES // nobs
    panels = sources.shape[1] // nfreq
    chunks = panels // CHUNK
    observers = jnp.tile(observer_table[:, observer_index], (1, share))
    pos = lax.dynamic_slice_in_dim(panel_pos, me * panels, panels, 1).T
    blade = lax.dynamic_slice_in_dim(panel_blade, me * panels, panels, 0)[None, :]
    steps = NF // share
    mine = steps // nfreq
    held = NCOMP // ngrp
    vmem = pl.BlockSpec(memory_space=pltpu.VMEM)
    got = pl.pallas_call(
        functools.partial(kernel, share, (nfreq, ngrp)),
        out_shape=jax.ShapeDtypeStruct((2 * held * mine, LANES), jnp.float32),
        in_specs=[vmem, pl.BlockSpec(memory_space=pl.ANY), vmem, vmem, vmem],
        out_specs=vmem,
        scratch_shapes=[
            pltpu.VMEM((steps, 2 * NCOMP, LANES), jnp.float32),
            pltpu.VMEM((2 * NF, CHUNK), jnp.float32),
            pltpu.VMEM((5, CHUNK, LANES), jnp.float32),
            pltpu.VMEM((2 * NCOMP, CHUNK), jnp.float32),
            pltpu.VMEM((STEPS, CHUNK, 2 * LANES), jnp.bfloat16),
            pltpu.VMEM((STEPS, CHUNK, 2 * LANES), jnp.bfloat16),
            pltpu.VMEM((chunks, NT, CHUNK), jnp.bfloat16),
            pltpu.VMEM((nfreq, mine, 2 * NCOMP, LANES), jnp.float32),
            pltpu.VMEM((mine, 2 * NCOMP, LANES), jnp.float32),
            pltpu.VMEM((ngrp, 2 * held * mine, LANES), jnp.float32),
            pltpu.VMEM((ngrp, 2 * held * mine, LANES), jnp.float32),
            pltpu.SemaphoreType.DMA((chunks,)),
            pltpu.SemaphoreType.DMA((chunks,)),
            pltpu.SemaphoreType.DMA,
            pltpu.SemaphoreType.DMA,
            pltpu.SemaphoreType.DMA,
            pltpu.SemaphoreType.DMA,
        ],
        compiler_params=pltpu.CompilerParams(collective_id=0, has_side_effects=True),
    )(transform_table(), sources, pos, blade, observers)
    got = got.reshape(held, 2, mine, share, nobs).transpose(2, 3, 0, 1, 4)
    return got.reshape(mine * share, held, 2, nobs)


def solution(mesh):
    in_specs = (P("freq", "grp"), P(None, "grp"), P("grp"), P(), P())
    out_specs = P("freq", "grp", None, None)
    return jax.shard_map(body, mesh=mesh, in_specs=in_specs, out_specs=out_specs, check_vma=False)
```

```python
import functools
import math

import jax
import jax.numpy as jnp
import numpy as np
from jax import lax
from jax.experimental import pallas as pl
from jax.experimental.pallas import tpu as pltpu
from jax.sharding import PartitionSpec as P

NT = 1024
NF = 512
NCOMP = 4
WAVE_STEP = 0.04
MESH = pl.DeviceIdType.MESH
LANES = 128
CHUNK = 256
STEPS = 8


def transform_table():
    turns = (np.arange(NF)[:, None] * np.arange(NT)[None, :]) % NT
    angle = 2.0 * math.pi / NT * turns
    values = np.stack([np.cos(angle), -np.sin(angle)], axis=1).reshape(2 * NF, NT)
    return jnp.asarray((values / math.sqrt(NT)).astype(np.float32)).astype(jnp.bfloat16)


def cos_sin(x):
    y = x * x
    cos = jnp.full_like(y, 1.0 / math.factorial(16))
    sin = jnp.full_like(y, -1.0 / math.factorial(15))
    for n in range(7, -1, -1):
        sign = 1.0 if n % 2 == 0 else -1.0
        cos = cos * y + sign / math.factorial(2 * n)
        if n < 7:
            sin = sin * y + sign / math.factorial(2 * n + 1)
    return cos, sin * x


def start_states(pos, obs, states, zero, share, turns, bits):
    rows = 32
    lane = lax.broadcasted_iota(jnp.int32, (rows, LANES), 1)
    j = (lane // (LANES // share)).astype(jnp.float32)
    for r in range(CHUNK // rows):
        at = slice(r * rows, (r + 1) * rows)
        d2 = None
        for axis in range(3):
            diff = obs[axis : axis + 1, :] - pos[at, axis : axis + 1]
            d2 = diff * diff if d2 is None else d2 + diff * diff
        d = jnp.sqrt(d2)
        amplitude = 0.25 / (math.pi * d)
        theta = WAVE_STEP * d
        cj, sj = cos_sin(j * theta)
        cs, ss = cos_sin(float(share) * theta)
        cj, sj = cj * amplitude, sj * amplitude
        c0, s0 = cj * cs + sj * ss, sj * cs - cj * ss
        zero[0, at, :], zero[1, at, :], zero[2, at, :], zero[3, at, :] = c0, cj, s0, sj
        states[4, at, :] = 2.0 * cs
        for _ in range((2 * STEPS).bit_length() - 1):
            cs, ss = cs * cs - ss * ss, 2.0 * cs * ss
        for b in range(bits):
            keep = lax.rem(lax.div(turns, 2**b), 2) == 1
            ct, st = jnp.where(keep, cs, 1.0), jnp.where(keep, ss, 0.0)
            c0, s0 = c0 * ct - s0 * st, s0 * ct + c0 * st
            cj, sj = cj * ct - sj * st, sj * ct + cj * st
            if b < bits - 1:
                cs, ss = cs * cs - ss * ss, 2.0 * cs * ss
        states[0, at, :], states[1, at, :], states[2, at, :], states[3, at, :] = c0, cj, s0, sj


def green_rows(states, green, r):
    at = pl.ds(r * 16, 16)
    c0, c1, s0, s1, t = (states[i, at, :] for i in range(5))
    for k in range(STEPS):
        green[k, at, :LANES] = c1.astype(jnp.bfloat16)
        green[k, at, LANES:] = s1.astype(jnp.bfloat16)
        c0, c1 = c1, t * c1 - c0
        s0, s1 = s1, t * s1 - s0
    states[0, at, :], states[1, at, :] = c0, c1
    states[2, at, :], states[3, at, :] = s0, s1


def contract(spec, mask, green, acc, step, k, share, first):
    sub = lax.broadcasted_iota(jnp.int32, (2 * NCOMP, CHUNK), 0)
    real_row = sub < NCOMP
    rows = []
    base = pl.multiple_of(step * 2 * share, 2 * share)
    pair = spec[pl.ds(base, 2 * share), :]
    for j in range(share):
        re = jnp.broadcast_to(pair[2 * j : 2 * j + 1, :], (2 * NCOMP, CHUNK))
        im = jnp.broadcast_to(pair[2 * j + 1 : 2 * j + 2, :], (2 * NCOMP, CHUNK))
        rows.append(jnp.where(real_row, re, im) * mask)
    weighted = jnp.concatenate(rows, axis=0).astype(jnp.bfloat16)
    prod = jnp.dot(weighted, green[k], preferred_element_type=jnp.float32)
    lane = lax.broadcasted_iota(jnp.int32, (2 * NCOMP, LANES), 1) // (LANES // share)
    even = prod[: 2 * NCOMP, :LANES]
    odd = prod[: 2 * NCOMP, LANES:]
    for j in range(1, share):
        block = prod[2 * NCOMP * j : 2 * NCOMP * (j + 1)]
        even = jnp.where(lane == j, block[:, :LANES], even)
        odd = jnp.where(lane == j, block[:, LANES:], odd)
    odd = jnp.concatenate([odd[NCOMP:], -odd[:NCOMP]], axis=0)
    total = even + odd
    if first:
        acc[step] = total
    else:
        acc[step] = acc[step] + total


def block_pair(spec, mask, now, acc, block, share, first, states, later):
    per = CHUNK // 16 // STEPS
    for k in range(STEPS):
        if now is not None:
            contract(spec, mask, now, acc, block * STEPS + k, k, share, first)
        if later is not None:
            for r in range(per):
                green_rows(states, later, k * per + r)


def phase(q, table_ref, block_of, blade, acc, spec, states, zero, mask, ga, gb, share, start, done):
    sub = lax.broadcasted_iota(jnp.int32, (2 * NCOMP, CHUNK), 0) % NCOMP
    mask[...] = jnp.where(blade == sub, 1.0, 0.0)
    block_pair(None, None, None, None, 0, share, False, states, ga)
    data = block_of(q)
    for r in range(4):
        part = pl.ds(r * (2 * NF // 4), 2 * NF // 4)
        spec[part, :] = (
            jnp.dot(table_ref[part, :], data, preferred_element_type=jnp.float32)
            .astype(jnp.bfloat16)
            .astype(jnp.float32)
        )
    pairs = NF // share // STEPS // 2

    def two(i, carry):
        m = mask[...]
        at = lax.rem(start + i, pairs)
        block_pair(spec, m, ga, acc, 2 * at, share, False, states, gb)

        @pl.when(at == pairs - 1)
        def _():
            states[0:4] = zero[...]

        block_pair(spec, m, gb, acc, 2 * at + 1, share, False, states, ga)
        done(q, at)
        return carry

    lax.fori_loop(0, pairs, two, 0)


def kernel(share, size, table_ref, src_ref, pos_ref, blade_ref, obs_ref, index_ref, out_ref, *scratch):
    (acc, spec, states, zero, mask, ga, gb, data, parts, total, zsend, zrecv, tail) = scratch[:13]
    (send_sem, recv_sem, part_send, part_recv, z_send, z_recv) = scratch[13:]
    nfreq, ngrp = size
    me, grp = lax.axis_index("freq"), lax.axis_index("grp")
    rows = src_ref.shape[0]
    panels = src_ref.shape[1] // nfreq
    chunks = panels // CHUNK
    mine = NF // share // nfreq

    def freq_peer(d):
        return lax.rem(me + d, nfreq)

    barrier = pltpu.get_barrier_semaphore()

    def greet(d, carry):
        pl.semaphore_signal(barrier, inc=1, device_id={"freq": freq_peer(d)}, device_id_type=MESH)
        return carry

    lax.fori_loop(1, nfreq, greet, 0)
    for d in range(1, ngrp):
        pl.semaphore_signal(barrier, inc=1, device_id={"grp": lax.rem(grp + d, ngrp)}, device_id_type=MESH)
    pl.semaphore_wait(barrier, nfreq + ngrp - 2)

    def columns(owner, q):
        return pl.ds(pl.multiple_of(owner * panels + q * CHUNK, CHUNK), CHUNK)

    landing = pl.ds(pl.multiple_of(me * rows, rows), rows)

    def send_chunk(q, carry):
        def to(d, carry):
            dest = freq_peer(d)
            pltpu.make_async_remote_copy(
                src_ref=src_ref.at[:, columns(dest, q)],
                dst_ref=data.at[q, landing, :],
                send_sem=send_sem.at[q],
                recv_sem=recv_sem.at[q],
                device_id={"freq": dest},
                device_id_type=MESH,
            ).start()
            return carry

        lax.fori_loop(1, nfreq, to, 0)
        pltpu.make_async_copy(src_ref.at[:, columns(me, q)], data.at[q, landing, :], recv_sem.at[q]).start()
        return carry

    lax.fori_loop(0, chunks, send_chunk, 0)
    acc[...] = jnp.zeros_like(acc)
    pairs = NF // share // STEPS // 2
    start = lax.rem(lax.div(me * mine, 2 * STEPS) + 1, pairs)
    index = jnp.concatenate([index_ref[...]] * share, axis=1)
    entry = lax.broadcasted_iota(jnp.int32, (obs_ref.shape[1], LANES), 0)
    chosen = jnp.where(entry == index, 1.0, 0.0)
    obs = jnp.dot(
        obs_ref[...], chosen, preferred_element_type=jnp.float32, precision=lax.Precision.HIGHEST
    )

    def prepare(q, carry):
        pos = jnp.concatenate([pos_ref[:, columns(me, q)], jnp.zeros((5, CHUNK), jnp.float32)], axis=0)
        start_states(pos.T, obs, states.at[q], zero.at[q], share, start, pairs.bit_length() - 1)
        return carry

    lax.fori_loop(0, chunks, prepare, 0)

    def block_of(q):
        pltpu.make_async_copy(data.at[q], data.at[q], recv_sem.at[q]).wait()
        return data[q]

    def done(q, i):
        ranges = 2 * STEPS // mine

        @pl.when(q == chunks - 1)
        def _():
            for r in range(ranges):
                dest = i * ranges + r

                @pl.when(dest != me)
                def _():
                    pltpu.make_async_remote_copy(
                        src_ref=acc.at[pl.ds(dest * mine, mine)],
                        dst_ref=parts.at[me],
                        send_sem=part_send,
                        recv_sem=part_recv,
                        device_id={"freq": dest},
                        device_id_type=MESH,
                    ).start()

    def step(q, carry):
        phase(q, table_ref, block_of, blade_ref[:, columns(me, q)], acc, spec, states.at[q], zero.at[q], mask, ga, gb, share, start, done)
        return carry

    lax.fori_loop(0, chunks, step, 0)

    parts[me] = acc[pl.ds(me * mine, mine)]
    others = parts.at[pl.ds(0, nfreq - 1)]
    pltpu.make_async_copy(others, others, part_recv).wait()
    total[...] = jnp.sum(parts[...], axis=0)
    held = NCOMP // ngrp
    for g in range(ngrp):
        for b in range(held):
            for c in range(2):
                at = (b * 2 + c) * mine
                zsend[g, at : at + mine, :] = total[:, c * NCOMP + g * held + b, :]
    for d in range(1, ngrp):
        dest = lax.rem(grp + d, ngrp)
        pltpu.make_async_remote_copy(
            src_ref=zsend.at[dest],
            dst_ref=zrecv.at[grp],
            send_sem=z_send,
            recv_sem=z_recv,
            device_id={"grp": dest},
            device_id_type=MESH,
        ).start()
    zrecv[grp] = zsend[grp]
    rest = zrecv.at[pl.ds(0, ngrp - 1)]
    pltpu.make_async_copy(rest, rest, z_recv).wait()
    final = jnp.sum(zrecv[...], axis=0)
    nobs = LANES // share
    for j in range(share):
        tail[j] = final[:, j * nobs : (j + 1) * nobs]
    for t in range(mine):
        for j in range(share):
            for b in range(held):
                for c in range(2):
                    row = (b * 2 + c) * mine + t
                    out_ref[t * share + j, b, c : c + 1, :] = tail[j, row : row + 1, :]
    pltpu.make_async_copy(rest, rest, z_send).wait()
    pltpu.make_async_copy(others, others, part_send).wait()

    def drain(q, carry):
        sent = data.at[q, pl.ds(0, (nfreq - 1) * rows), :]
        pltpu.make_async_copy(sent, sent, send_sem.at[q]).wait()
        return carry

    lax.fori_loop(0, chunks, drain, 0)


def body(sources, panel_pos, panel_blade, observer_table, observer_index):
    nfreq, ngrp = lax.axis_size("freq"), lax.axis_size("grp")
    nobs = observer_index.shape[0]
    share = LANES // nobs
    panels = sources.shape[1] // nfreq
    chunks = panels // CHUNK
    steps = NF // share
    mine = steps // nfreq
    held = NCOMP // ngrp
    vmem = pl.BlockSpec(memory_space=pltpu.VMEM)
    f32 = jnp.float32
    return pl.pallas_call(
        functools.partial(kernel, share, (nfreq, ngrp)),
        out_shape=jax.ShapeDtypeStruct((NF // nfreq, held, 2, nobs), f32),
        in_specs=[vmem, pl.BlockSpec(memory_space=pl.ANY)] + [vmem] * 4,
        out_specs=vmem,
        scratch_shapes=[
            pltpu.VMEM((steps, 2 * NCOMP, LANES), f32),
            pltpu.VMEM((2 * NF, CHUNK), f32),
            pltpu.VMEM((chunks, 5, CHUNK, LANES), f32),
            pltpu.VMEM((chunks, 4, CHUNK, LANES), f32),
            pltpu.VMEM((2 * NCOMP, CHUNK), f32),
            pltpu.VMEM((STEPS, CHUNK, 2 * LANES), jnp.bfloat16),
            pltpu.VMEM((STEPS, CHUNK, 2 * LANES), jnp.bfloat16),
            pltpu.VMEM((chunks, NT, CHUNK), jnp.bfloat16),
            pltpu.VMEM((nfreq, mine, 2 * NCOMP, LANES), f32),
            pltpu.VMEM((mine, 2 * NCOMP, LANES), f32),
            pltpu.VMEM((ngrp, 2 * held * mine, LANES), f32),
            pltpu.VMEM((ngrp, 2 * held * mine, LANES), f32),
            pltpu.VMEM((share, 2 * held * mine, nobs), f32),
            pltpu.SemaphoreType.DMA((chunks,)),
            pltpu.SemaphoreType.DMA((chunks,)),
            pltpu.SemaphoreType.DMA,
            pltpu.SemaphoreType.DMA,
            pltpu.SemaphoreType.DMA,
            pltpu.SemaphoreType.DMA,
        ],
        compiler_params=pltpu.CompilerParams(collective_id=0, has_side_effects=True),
    )(transform_table(), sources, panel_pos, panel_blade[None, :], observer_table, observer_index[None, :])


def solution(mesh):
    in_specs = (P("freq", "grp"), P(None, "grp"), P("grp"), P(), P())
    out_specs = P("freq", "grp", None, None)
    return jax.shard_map(body, mesh=mesh, in_specs=in_specs, out_specs=out_specs, check_vma=False)
```

```python
import functools
import math

import jax
import jax.numpy as jnp
import numpy as np
from jax import lax
from jax.experimental import pallas as pl
from jax.experimental.pallas import tpu as pltpu
from jax.sharding import PartitionSpec as P

NT = 1024
NF = 512
NCOMP = 4
WAVE_STEP = 0.04
MESH = pl.DeviceIdType.MESH
LANES = 128
CHUNK = 256
STEPS = 8


def transform_table():
    turns = (np.arange(NF)[:, None] * np.arange(NT)[None, :]) % NT
    angle = 2.0 * math.pi / NT * turns
    values = np.stack([np.cos(angle), -np.sin(angle)], axis=1).reshape(2 * NF, NT)
    return jnp.asarray((values / math.sqrt(NT)).astype(np.float32)).astype(jnp.bfloat16)


def cos_sin(x):
    y = x * x
    cos = jnp.full_like(y, 1.0 / math.factorial(16))
    sin = jnp.full_like(y, -1.0 / math.factorial(15))
    for n in range(7, -1, -1):
        sign = 1.0 if n % 2 == 0 else -1.0
        cos = cos * y + sign / math.factorial(2 * n)
        if n < 7:
            sin = sin * y + sign / math.factorial(2 * n + 1)
    return cos, sin * x


def start_states(pos, obs, states, zero, share, turns, bits):
    rows = 32
    lane = lax.broadcasted_iota(jnp.int32, (rows, LANES), 1)
    j = (lane // (LANES // share)).astype(jnp.float32)
    for r in range(CHUNK // rows):
        at = slice(r * rows, (r + 1) * rows)
        d2 = None
        for axis in range(3):
            diff = obs[axis : axis + 1, :] - pos[at, axis : axis + 1]
            d2 = diff * diff if d2 is None else d2 + diff * diff
        d = jnp.sqrt(d2)
        amplitude = 0.25 / (math.pi * d)
        theta = WAVE_STEP * d
        cj, sj = cos_sin(j * theta)
        cs, ss = cos_sin(float(share) * theta)
        cj, sj = cj * amplitude, sj * amplitude
        c0, s0 = cj * cs + sj * ss, sj * cs - cj * ss
        zero[0, at, :], zero[1, at, :], zero[2, at, :], zero[3, at, :] = c0, cj, s0, sj
        states[4, at, :] = 2.0 * cs
        for _ in range((2 * STEPS).bit_length() - 1):
            cs, ss = cs * cs - ss * ss, 2.0 * cs * ss
        for b in range(bits):
            keep = lax.rem(lax.div(turns, 2**b), 2) == 1
            ct, st = jnp.where(keep, cs, 1.0), jnp.where(keep, ss, 0.0)
            c0, s0 = c0 * ct - s0 * st, s0 * ct + c0 * st
            cj, sj = cj * ct - sj * st, sj * ct + cj * st
            if b < bits - 1:
                cs, ss = cs * cs - ss * ss, 2.0 * cs * ss
        states[0, at, :], states[1, at, :], states[2, at, :], states[3, at, :] = c0, cj, s0, sj


def green_rows(states, green, r):
    at = pl.ds(r * 16, 16)
    c0, c1, s0, s1, t = (states[i, at, :] for i in range(5))
    for k in range(STEPS):
        green[k, at, :LANES] = c1.astype(jnp.bfloat16)
        green[k, at, LANES:] = s1.astype(jnp.bfloat16)
        c0, c1 = c1, t * c1 - c0
        s0, s1 = s1, t * s1 - s0
    states[0, at, :], states[1, at, :] = c0, c1
    states[2, at, :], states[3, at, :] = s0, s1


def contract(spec, mask, green, acc, step, k, share, first):
    sub = lax.broadcasted_iota(jnp.int32, (2 * NCOMP, CHUNK), 0)
    real_row = sub < NCOMP
    rows = []
    base = pl.multiple_of(step * 2 * share, 2 * share)
    pair = spec[pl.ds(base, 2 * share), :]
    for j in range(share):
        re = jnp.broadcast_to(pair[2 * j : 2 * j + 1, :], (2 * NCOMP, CHUNK))
        im = jnp.broadcast_to(pair[2 * j + 1 : 2 * j + 2, :], (2 * NCOMP, CHUNK))
        rows.append(jnp.where(real_row, re, im) * mask)
    weighted = jnp.concatenate(rows, axis=0).astype(jnp.bfloat16)
    prod = jnp.dot(weighted, green[k], preferred_element_type=jnp.float32)
    lane = lax.broadcasted_iota(jnp.int32, (2 * NCOMP, LANES), 1) // (LANES // share)
    even = prod[: 2 * NCOMP, :LANES]
    odd = prod[: 2 * NCOMP, LANES:]
    for j in range(1, share):
        block = prod[2 * NCOMP * j : 2 * NCOMP * (j + 1)]
        even = jnp.where(lane == j, block[:, :LANES], even)
        odd = jnp.where(lane == j, block[:, LANES:], odd)
    odd = jnp.concatenate([odd[NCOMP:], -odd[:NCOMP]], axis=0)
    total = even + odd
    if first:
        acc[step] = total
    else:
        acc[step] = acc[step] + total


def block_pair(spec, mask, now, acc, block, share, first, states, later):
    per = CHUNK // 16 // STEPS
    for k in range(STEPS):
        if now is not None:
            contract(spec, mask, now, acc, block * STEPS + k, k, share, first)
        if later is not None:
            for r in range(per):
                green_rows(states, later, k * per + r)


def phase(q, table_ref, block_of, blade, acc, spec, states, zero, mask, ga, gb, share, start, done):
    sub = lax.broadcasted_iota(jnp.int32, (2 * NCOMP, CHUNK), 0) % NCOMP
    mask[...] = jnp.where(blade == sub, 1.0, 0.0)
    block_pair(None, None, None, None, 0, share, False, states, ga)
    data = block_of(q)
    for r in range(4):
        part = pl.ds(r * (2 * NF // 4), 2 * NF // 4)
        spec[part, :] = (
            jnp.dot(table_ref[part, :], data, preferred_element_type=jnp.float32)
            .astype(jnp.bfloat16)
            .astype(jnp.float32)
        )
    pairs = NF // share // STEPS // 2

    def two(i, carry):
        m = mask[...]
        at = lax.rem(start + i, pairs)
        block_pair(spec, m, ga, acc, 2 * at, share, False, states, gb)

        @pl.when(at == pairs - 1)
        def _():
            states[0:4] = zero[...]

        @pl.when(at < pairs)
        def _():
            block_pair(spec, mask[...], gb, acc, 2 * at + 1, share, False, states, ga)

        done(q, at)
        return carry

    lax.fori_loop(0, pairs, two, 0)


def kernel(share, size, table_ref, src_ref, pos_ref, blade_ref, obs_ref, index_ref, out_ref, *scratch):
    (acc, spec, states, zero, mask, ga, gb, data, parts, total, zsend, zrecv, tail) = scratch[:13]
    (send_sem, recv_sem, part_send, part_recv, z_send, z_recv) = scratch[13:]
    nfreq, ngrp = size
    me, grp = lax.axis_index("freq"), lax.axis_index("grp")
    rows = src_ref.shape[0]
    panels = src_ref.shape[1] // nfreq
    chunks = panels // CHUNK
    mine = NF // share // nfreq

    def freq_peer(d):
        return lax.rem(me + d, nfreq)

    barrier = pltpu.get_barrier_semaphore()

    def greet(d, carry):
        pl.semaphore_signal(barrier, inc=1, device_id={"freq": freq_peer(d)}, device_id_type=MESH)
        return carry

    lax.fori_loop(1, nfreq, greet, 0)
    for d in range(1, ngrp):
        pl.semaphore_signal(barrier, inc=1, device_id={"grp": lax.rem(grp + d, ngrp)}, device_id_type=MESH)
    pl.semaphore_wait(barrier, nfreq + ngrp - 2)

    def columns(owner, q):
        return pl.ds(pl.multiple_of(owner * panels + q * CHUNK, CHUNK), CHUNK)

    landing = pl.ds(pl.multiple_of(me * rows, rows), rows)

    def send_chunk(q, carry):
        def to(d, carry):
            dest = freq_peer(d)
            pltpu.make_async_remote_copy(
                src_ref=src_ref.at[:, columns(dest, q)],
                dst_ref=data.at[q, landing, :],
                send_sem=send_sem.at[q],
                recv_sem=recv_sem.at[q],
                device_id={"freq": dest},
                device_id_type=MESH,
            ).start()
            return carry

        lax.fori_loop(1, nfreq, to, 0)
        pltpu.make_async_copy(src_ref.at[:, columns(me, q)], data.at[q, landing, :], recv_sem.at[q]).start()
        return carry

    lax.fori_loop(0, chunks, send_chunk, 0)
    acc[...] = jnp.zeros_like(acc)
    pairs = NF // share // STEPS // 2
    start = lax.rem(lax.div(me * mine, 2 * STEPS) + 1, pairs)
    index = jnp.concatenate([index_ref[...]] * share, axis=1)
    entry = lax.broadcasted_iota(jnp.int32, (obs_ref.shape[1], LANES), 0)
    chosen = jnp.where(entry == index, 1.0, 0.0)
    obs = jnp.dot(
        obs_ref[...], chosen, preferred_element_type=jnp.float32, precision=lax.Precision.HIGHEST
    )

    def prepare(q, carry):
        pos = jnp.concatenate([pos_ref[:, columns(me, q)], jnp.zeros((5, CHUNK), jnp.float32)], axis=0)
        start_states(pos.T, obs, states.at[q], zero.at[q], share, start, pairs.bit_length() - 1)
        return carry

    lax.fori_loop(0, chunks, prepare, 0)

    def block_of(q):
        pltpu.make_async_copy(data.at[q], data.at[q], recv_sem.at[q]).wait()
        return data[q]

    def done(q, i):
        ranges = 2 * STEPS // mine

        @pl.when(q == chunks - 1)
        def _():
            for r in range(ranges):
                dest = i * ranges + r

                @pl.when(dest != me)
                def _():
                    pltpu.make_async_remote_copy(
                        src_ref=acc.at[pl.ds(dest * mine, mine)],
                        dst_ref=parts.at[me],
                        send_sem=part_send,
                        recv_sem=part_recv,
                        device_id={"freq": dest},
                        device_id_type=MESH,
                    ).start()

    def step(q, carry):
        phase(q, table_ref, block_of, blade_ref[:, columns(me, q)], acc, spec, states.at[q], zero.at[q], mask, ga, gb, share, start, done)
        return carry

    lax.fori_loop(0, chunks, step, 0)

    parts[me] = acc[pl.ds(me * mine, mine)]
    others = parts.at[pl.ds(0, nfreq - 1)]
    pltpu.make_async_copy(others, others, part_recv).wait()
    total[...] = jnp.sum(parts[...], axis=0)
    held = NCOMP // ngrp
    for g in range(ngrp):
        for b in range(held):
            for c in range(2):
                at = (b * 2 + c) * mine
                zsend[g, at : at + mine, :] = total[:, c * NCOMP + g * held + b, :]
    for d in range(1, ngrp):
        dest = lax.rem(grp + d, ngrp)
        pltpu.make_async_remote_copy(
            src_ref=zsend.at[dest],
            dst_ref=zrecv.at[grp],
            send_sem=z_send,
            recv_sem=z_recv,
            device_id={"grp": dest},
            device_id_type=MESH,
        ).start()
    zrecv[grp] = zsend[grp]
    rest = zrecv.at[pl.ds(0, ngrp - 1)]
    pltpu.make_async_copy(rest, rest, z_recv).wait()
    final = jnp.sum(zrecv[...], axis=0)
    nobs = LANES // share
    for j in range(share):
        tail[j] = final[:, j * nobs : (j + 1) * nobs]
    for t in range(mine):
        for j in range(share):
            for b in range(held):
                for c in range(2):
                    row = (b * 2 + c) * mine + t
                    out_ref[t * share + j, b, c : c + 1, :] = tail[j, row : row + 1, :]
    pltpu.make_async_copy(rest, rest, z_send).wait()
    pltpu.make_async_copy(others, others, part_send).wait()

    def drain(q, carry):
        sent = data.at[q, pl.ds(0, (nfreq - 1) * rows), :]
        pltpu.make_async_copy(sent, sent, send_sem.at[q]).wait()
        return carry

    lax.fori_loop(0, chunks, drain, 0)


def body(sources, panel_pos, panel_blade, observer_table, observer_index):
    nfreq, ngrp = lax.axis_size("freq"), lax.axis_size("grp")
    nobs = observer_index.shape[0]
    share = LANES // nobs
    panels = sources.shape[1] // nfreq
    chunks = panels // CHUNK
    steps = NF // share
    mine = steps // nfreq
    held = NCOMP // ngrp
    vmem = pl.BlockSpec(memory_space=pltpu.VMEM)
    f32 = jnp.float32
    return pl.pallas_call(
        functools.partial(kernel, share, (nfreq, ngrp)),
        out_shape=jax.ShapeDtypeStruct((NF // nfreq, held, 2, nobs), f32),
        in_specs=[vmem, pl.BlockSpec(memory_space=pl.ANY)] + [vmem] * 4,
        out_specs=vmem,
        scratch_shapes=[
            pltpu.VMEM((steps, 2 * NCOMP, LANES), f32),
            pltpu.VMEM((2 * NF, CHUNK), f32),
            pltpu.VMEM((chunks, 5, CHUNK, LANES), f32),
            pltpu.VMEM((chunks, 4, CHUNK, LANES), f32),
            pltpu.VMEM((2 * NCOMP, CHUNK), f32),
            pltpu.VMEM((STEPS, CHUNK, 2 * LANES), jnp.bfloat16),
            pltpu.VMEM((STEPS, CHUNK, 2 * LANES), jnp.bfloat16),
            pltpu.VMEM((chunks, NT, CHUNK), jnp.bfloat16),
            pltpu.VMEM((nfreq, mine, 2 * NCOMP, LANES), f32),
            pltpu.VMEM((mine, 2 * NCOMP, LANES), f32),
            pltpu.VMEM((ngrp, 2 * held * mine, LANES), f32),
            pltpu.VMEM((ngrp, 2 * held * mine, LANES), f32),
            pltpu.VMEM((share, 2 * held * mine, nobs), f32),
            pltpu.SemaphoreType.DMA((chunks,)),
            pltpu.SemaphoreType.DMA((chunks,)),
            pltpu.SemaphoreType.DMA,
            pltpu.SemaphoreType.DMA,
            pltpu.SemaphoreType.DMA,
            pltpu.SemaphoreType.DMA,
        ],
        compiler_params=pltpu.CompilerParams(collective_id=0, has_side_effects=True),
    )(transform_table(), sources, panel_pos, panel_blade[None, :], observer_table, observer_index[None, :])


def solution(mesh):
    in_specs = (P("freq", "grp"), P(None, "grp"), P("grp"), P(), P())
    out_specs = P("freq", "grp", None, None)
    return jax.shard_map(body, mesh=mesh, in_specs=in_specs, out_specs=out_specs, check_vma=False)
```
